32 devices in a mesh: data: 1 (over z), dap2: 4 (over y), dap: 8 (over x, core).
Axes of the slice: x: 4, y: 4, z: 1, core: 2. Of those that a mesh axis runs over, the one named last changes fastest.
The devices are a block of a 4x4x8 slice.
Arguments:
- pair_rep: bfloat16 [1024, 1024, 128], P(('data', 'dap2', 'dap'))
- pair_mask: int32 [1024, 1024], P(('data', 'dap2', 'dap'))
- norm_in: bfloat16 [3, 2, 2, 128], replicated
- norm_out: bfloat16 [3, 2, 2, 128], replicated
- w_ab: bfloat16 [3, 2, 128, 512], replicated
- w_gate: bfloat16 [3, 2, 128, 128], replicated
- w_out: bfloat16 [3, 2, 128, 128], replicated
Outputs:
- output: bfloat16 [1024, 1024, 128], P(('data', 'dap2', 'dap'))
All inputs are finite; a program needn't handle non-finite values.
Results may differ from the reference program's by a relative error of at most 0.00996528.
Values are sent between devices in bfloat16 or wider.
A program may use at most 768 MiB of HBM per device.

```python
import jax
import jax.numpy as jnp
from jax import lax

N_RES = 1024
C_PAIR = 128
C_HID = 128
N_LAYERS = 3
LN_EPS = 1e-5


def setup_inputs(seed: int = 0, part: int = 0) -> dict:
    base_key = jax.random.key(seed)
    part_key = jax.random.fold_in(base_key, part)
    pair_key, mask_key = jax.random.split(part_key)
    weight_keys = jax.random.split(jax.random.key(seed + 17), 5)
    pair_rep = jax.random.normal(pair_key, (N_RES, N_RES, C_PAIR), jnp.float32).astype(jnp.bfloat16)
    keep_res = (jax.random.randint(mask_key, (N_RES,), 0, 16) != 0).astype(jnp.int32)
    pair_mask = keep_res[:, None] * keep_res[None, :]
    norm_base = jnp.array([1.0, 0.0], jnp.float32)[:, None]
    norm_in = (norm_base + 0.3 * jax.random.normal(weight_keys[0], (N_LAYERS, 2, 2, C_PAIR), jnp.float32)).astype(jnp.bfloat16)
    norm_out = (norm_base + 0.3 * jax.random.normal(weight_keys[1], (N_LAYERS, 2, 2, C_HID), jnp.float32)).astype(jnp.bfloat16)
    w_ab = (jax.random.normal(weight_keys[2], (N_LAYERS, 2, C_PAIR, 4 * C_HID), jnp.float32) * C_PAIR ** -0.5).astype(jnp.bfloat16)
    w_gate = (jax.random.normal(weight_keys[3], (N_LAYERS, 2, C_PAIR, C_PAIR), jnp.float32) * C_PAIR ** -0.5).astype(jnp.bfloat16)
    w_out = (jax.random.normal(weight_keys[4], (N_LAYERS, 2, C_HID, C_PAIR), jnp.float32) * (0.5 * C_HID ** -0.5)).astype(jnp.bfloat16)
    return {"pair_rep": pair_rep, "pair_mask": pair_mask, "norm_in": norm_in, "norm_out": norm_out, "w_ab": w_ab, "w_gate": w_gate, "w_out": w_out}


def layer_norm(values, gain_vec, shift_vec, norm_axis):
    mean_val = jnp.mean(values, axis=norm_axis, keepdims=True)
    centered = values - mean_val
    var_val = jnp.mean(centered * centered, axis=norm_axis, keepdims=True)
    return centered * lax.rsqrt(var_val + LN_EPS) * gain_vec + shift_vec


def tri_update(pair_cur, mask_f, norm_in, norm_out, w_ab, w_gate, w_out, outgoing):
    gain_in = norm_in[0].astype(jnp.float32)
    shift_in = norm_in[1].astype(jnp.float32)
    gain_out = norm_out[0].astype(jnp.float32)
    shift_out = norm_out[1].astype(jnp.float32)

    def row_inputs(row_args):
        x_row = layer_norm(row_args[0].astype(jnp.float32), gain_in, shift_in, -1).astype(jnp.bfloat16)
        proj_row = jnp.dot(x_row, w_ab, preferred_element_type=jnp.float32).reshape(N_RES, 4, C_HID)
        a_row = (row_args[1] * jax.nn.sigmoid(proj_row[:, 1]) * proj_row[:, 0]).astype(jnp.bfloat16)
        b_row = (row_args[1] * jax.nn.sigmoid(proj_row[:, 3]) * proj_row[:, 2]).astype(jnp.bfloat16)
        return a_row, b_row

    def out_channel(ab_pair):
        return jnp.dot(ab_pair[0], ab_pair[1].T, preferred_element_type=jnp.float32).astype(jnp.bfloat16)

    def in_channel(ab_pair):
        return jnp.dot(ab_pair[0].T, ab_pair[1], preferred_element_type=jnp.float32).astype(jnp.bfloat16)

    def row_output(row_args):
        pair_f = row_args[0].astype(jnp.float32)
        x_row = layer_norm(pair_f, gain_in, shift_in, -1).astype(jnp.bfloat16)
        y_row = layer_norm(row_args[1].astype(jnp.float32), gain_out, shift_out, -1).astype(jnp.bfloat16)
        update_val = jnp.dot(y_row, w_out, preferred_element_type=jnp.float32)
        gate_val = jax.nn.sigmoid(jnp.dot(x_row, w_gate, preferred_element_type=jnp.float32))
        return (pair_f + gate_val * update_val).astype(jnp.bfloat16)

    a_val, b_val = lax.map(row_inputs, (pair_cur, mask_f))
    channel_fn = out_channel if outgoing else in_channel
    tri_out = lax.map(channel_fn, (jnp.transpose(a_val, (2, 0, 1)), jnp.transpose(b_val, (2, 0, 1))))
    return lax.map(row_output, (pair_cur, jnp.transpose(tri_out, (1, 2, 0))))


def reference(pair_rep, pair_mask, norm_in, norm_out, w_ab, w_gate, w_out):
    mask_f = pair_mask.astype(jnp.float32)[:, :, None]

    def layer_step(pair_cur, params):
        pair_cur = tri_update(pair_cur, mask_f, params[0][0], params[1][0], params[2][0], params[3][0], params[4][0], True)
        pair_cur = tri_update(pair_cur, mask_f, params[0][1], params[1][1], params[2][1], params[3][1], params[4][1], False)
        return pair_cur, None

    return lax.scan(layer_step, pair_rep, (norm_in, norm_out, w_ab, w_gate, w_out))[0]
```

```python
import functools

import jax
import jax.numpy as jnp
from jax import lax
from jax.experimental import pallas as pl
from jax.experimental.pallas import tpu as pltpu
from jax.sharding import PartitionSpec as P

LN_EPS = 1e-5
ROW_AXES = ("dap2", "dap")
ALL_ROWS = ("data", "dap2", "dap")
CHUNKS = 2
ROWS = 16
LANES = 128
F32, BF16 = jnp.float32, jnp.bfloat16


def channel_norm(values, gain, shift):
    mean_val = jnp.mean(values, axis=0, keepdims=True)
    centered = values - mean_val
    var_val = jnp.mean(centered * centered, axis=0, keepdims=True)
    return centered * lax.rsqrt(var_val + LN_EPS) * gain + shift


def sigmoid(values):
    return 1.0 / (1.0 + jnp.exp(-values))


def local_kernel(*refs, first, last, parts):
    refs = list(refs)
    z_ref = refs.pop(0)
    if not first:
        t_ref, gain_in, shift_in, gain_out, shift_out, wg_ref, wo_ref = refs[:7]
        refs = refs[7:]
    if not last:
        mask_ref, gain_nx, shift_nx, wab_ref = refs[:4]
        refs = refs[4:]
    if last and parts > 1:
        refs.pop(0)
    z_out = refs.pop(0)
    ab_out = None if last else refs.pop(0)
    t_scr = None if first else refs.pop(0)
    ab_scr = None if last else refs.pop(0)
    rows = z_ref.shape[0]
    cols = z_out.shape[1] if last else z_out.shape[2]
    blocks = cols // LANES
    hid = wab_ref.shape[0] // 4 if not last else wo_ref.shape[1]

    if not first:
        stride_t = t_scr.shape[1] // hid
        for blk in range(blocks):
            lanes = pl.ds(blk * LANES, LANES)

            def add_up(c, total):
                return total + t_ref[c, :, lanes].astype(F32)

            mean_val = lax.fori_loop(0, hid, add_up, jnp.zeros((rows, LANES), F32), unroll=8) * (1.0 / hid)

            def add_sq(c, total):
                centered = t_ref[c, :, lanes].astype(F32) - mean_val
                return total + centered * centered

            var_val = lax.fori_loop(0, hid, add_sq, jnp.zeros((rows, LANES), F32), unroll=8) * (1.0 / hid)
            scale = lax.rsqrt(var_val + LN_EPS)

            def put(c, carry):
                start = pl.multiple_of(c * stride_t, 8)
                t_scr[blk, pl.ds(start, rows), :] = (t_ref[c, :, lanes].astype(F32) - mean_val) * scale
                return carry

            lax.fori_loop(0, hid, put, 0, unroll=8)

    def one_row(r, carry):
        if first:
            z_val = z_ref[r].astype(F32).T.astype(BF16)
        else:
            z_val = z_ref[r]
        z_f = z_val.astype(F32)
        if not first:
            x_ln = channel_norm(z_f, gain_in[...], shift_in[...]).astype(BF16)
            t_n = [t_scr[blk, pl.ds(r, hid, stride=stride_t), :] for blk in range(blocks)]
            t_n = jnp.concatenate(t_n, axis=1) if blocks > 1 else t_n[0]
            y_ln = (t_n * gain_out[...] + shift_out[...]).astype(BF16)
            update_val = jnp.dot(wo_ref[...], y_ln, preferred_element_type=F32)
            gate_val = sigmoid(jnp.dot(wg_ref[...], x_ln, preferred_element_type=F32))
            z_f = z_f + gate_val * update_val
            if last:
                z_out[r] = z_f.T.astype(BF16)
                return carry
            z_val = z_f.astype(BF16)
            z_f = z_val.astype(F32)
        z_out[r] = z_val
        x_nx = channel_norm(z_f, gain_nx[...], shift_nx[...]).astype(BF16)
        m_row = mask_ref[pl.ds(r, 1), :].astype(F32)
        stride_ab = ab_scr.shape[1] // rows
        for half in range(2):
            proj = jnp.dot(wab_ref[pl.ds(half * 2 * hid, 2 * hid), :], x_nx, preferred_element_type=F32)
            val = m_row * sigmoid(proj[hid:]) * proj[:hid]
            start = pl.multiple_of(r * stride_ab + half * hid, 8)
            for blk in range(blocks):
                ab_scr[blk, pl.ds(start, hid), :] = val[:, blk * LANES : (blk + 1) * LANES]
        return carry

    lax.fori_loop(0, rows, one_row, 0)

    if not last:
        dests, per_dest = ab_out.shape[0], ab_out.shape[1] // 2
        stride_ab = ab_scr.shape[1] // rows

        def send_rows(d, carry):
            for half in range(2):
                for e in range(per_dest):
                    for blk in range(blocks):
                        val = ab_scr[blk, pl.ds(half * hid + d * per_dest + e, rows, stride=stride_ab), :]
                        ab_out[d, half * per_dest + e, :, pl.ds(blk * LANES, LANES)] = val.astype(BF16)
            return carry

        lax.fori_loop(0, dests, send_rows, 0)


def local_call(z_in, t_in, mask_loc, prev, nxt, chunk, out_full, n_dev, width):
    first, last = prev is None, nxt is None
    rows_loc = mask_loc.shape[0]
    chan = z_in.shape[2] if first else z_in.shape[1]
    hid = chan if first else t_in.shape[0]
    wb = min(2 * LANES, width)
    nw = width // wb
    grid = (rows_loc // ROWS, nw)
    whole = lambda arr: pl.BlockSpec(arr.shape, lambda i, j: (0,) * arr.ndim)
    args, specs = [z_in], []
    if first:
        specs.append(pl.BlockSpec((ROWS, wb, chan), lambda i, j: (i, chunk * nw + j, 0)))
    else:
        specs.append(pl.BlockSpec((ROWS, chan, wb), lambda i, j: (i, 0, j)))
        args.append(t_in)
        specs.append(pl.BlockSpec((hid, ROWS, wb), lambda i, j: (0, i, j)))
        args += list(prev)
        specs += [whole(arr) for arr in prev]
    if not last:
        args.append(mask_loc)
        specs.append(pl.BlockSpec((ROWS, wb), lambda i, j: (i, chunk * nw + j)))
        args += list(nxt)
        specs += [whole(arr) for arr in nxt]
    alias = {}
    if last:
        parts = 1 if out_full is None else 2
        if out_full is not None:
            alias = {len(args): 0}
            args.append(out_full)
            specs.append(pl.BlockSpec(memory_space=pl.ANY))
        out_shape = jax.ShapeDtypeStruct((rows_loc, mask_loc.shape[1], chan), BF16)
        out_specs = pl.BlockSpec((ROWS, wb, chan), lambda i, j: (i, chunk * nw + j, 0))
    else:
        parts = 1
        per = 2 * hid // n_dev
        out_shape = (
            jax.ShapeDtypeStruct((rows_loc, chan, width), BF16),
            jax.ShapeDtypeStruct((n_dev, per, rows_loc, width), BF16),
        )
        out_specs = (
            pl.BlockSpec((ROWS, chan, wb), lambda i, j: (i, 0, j)),
            pl.BlockSpec((n_dev, per, ROWS, wb), lambda i, j: (0, 0, i, j)),
        )
    scratch = []
    if not first:
        scratch.append(pltpu.VMEM((wb // LANES, hid * (ROWS + 8), LANES), F32))
    if not last:
        scratch.append(pltpu.VMEM((wb // LANES, ROWS * (2 * hid + 8), LANES), F32))
    pos = rows_loc * width
    flops = 2 * pos * chan * ((0 if first else 2 * hid) + (0 if last else 4 * hid))
    return pl.pallas_call(
        functools.partial(local_kernel, first=first, last=last, parts=parts),
        grid=grid,
        in_specs=specs,
        out_specs=out_specs,
        out_shape=out_shape,
        scratch_shapes=scratch,
        input_output_aliases=alias,
        compiler_params=pltpu.CompilerParams(vmem_limit_bytes=60 * 2**20),
        cost_estimate=pl.CostEstimate(flops=flops, bytes_accessed=6 * pos * chan, transcendentals=0),
        name=f"local_{chunk}",
    )(*args)


def out_kernel(*refs, chunks):
    t_ref = refs[-1]
    total = None
    for p in range(chunks):
        a_val = refs[p][...].reshape(-1, refs[p].shape[-1])
        b_val = refs[chunks + p][...].reshape(-1, refs[chunks + p].shape[-1])
        part = lax.dot_general(a_val, b_val, (((1,), (1,)), ((), ())), preferred_element_type=F32)
        total = part if total is None else total + part
    t_ref[...] = total.astype(BF16).reshape(t_ref.shape)


def in_kernel(*refs, chunks):
    b_ref, t_ref = refs[chunks], refs[-1]
    b_val = b_ref[...].reshape(-1, b_ref.shape[-1])
    n_dev, _, rows, _ = t_ref.shape
    share = n_dev // chunks
    for p in range(chunks):
        a_val = refs[p][...].reshape(-1, refs[p].shape[-1])
        part = lax.dot_general(a_val, b_val, (((0,), (0,)), ((), ())), preferred_element_type=F32)
        t_ref[p * share : (p + 1) * share] = part.astype(BF16).reshape(share, 1, rows, t_ref.shape[-1])


def tri_call(ab_cols, q, outgoing):
    chunks = len(ab_cols)
    n_dev, per, rows, width = ab_cols[0].shape
    per //= 2
    a_spec = pl.BlockSpec((n_dev, 1, rows, width), lambda c: (0, c, 0, 0))
    if outgoing:
        body = out_kernel
        args = list(ab_cols) + list(ab_cols)
        b_spec = pl.BlockSpec((n_dev // chunks, 1, rows, width), lambda c: (q, per + c, 0, 0))
        specs = [a_spec] * chunks + [b_spec] * chunks
    else:
        body = in_kernel
        args = list(ab_cols) + [ab_cols[q]]
        specs = [a_spec] * chunks + [pl.BlockSpec((n_dev, 1, rows, width), lambda c: (0, per + c, 0, 0))]
    size = n_dev * rows
    return pl.pallas_call(
        functools.partial(body, chunks=chunks),
        grid=(per,),
        in_specs=specs,
        out_specs=pl.BlockSpec((n_dev, 1, rows, width), lambda c: (0, c, 0, 0)),
        out_shape=jax.ShapeDtypeStruct((n_dev, per, rows, width), BF16),
        compiler_params=pltpu.CompilerParams(vmem_limit_bytes=60 * 2**20),
        cost_estimate=pl.CostEstimate(
            flops=2 * per * size * size * width, bytes_accessed=6 * per * size * width, transcendentals=0
        ),
        name=f"tri_{q}",
    )(*args)


def exchange(blocks):
    flat = blocks.reshape(blocks.shape[0], -1, blocks.shape[-1])
    return lax.all_to_all(flat, ROW_AXES, 0, 0, tiled=True).reshape(blocks.shape)


def solution(mesh):
    n_dev = mesh.shape["dap2"] * mesh.shape["dap"]
    row_spec = P(ALL_ROWS, None, None)
    mask_spec = P(ALL_ROWS, None)

    def local_stack(pair_rep, pair_mask, norm_in, norm_out, w_ab, w_gate, w_out):
        width = pair_rep.shape[1] // CHUNKS
        wb = min(2 * LANES, width)

        def spread(vec):
            return jnp.broadcast_to(vec.astype(F32)[:, None], (vec.shape[0], wb))

        steps = [(layer, upd) for layer in range(w_ab.shape[0]) for upd in range(2)]

        def before(s):
            l, u = steps[s]
            return (spread(norm_in[l, u, 0]), spread(norm_in[l, u, 1]), w_ab[l, u].T)

        def after(s):
            l, u = steps[s]
            gains = tuple(spread(v) for v in (norm_in[l, u, 0], norm_in[l, u, 1], norm_out[l, u, 0], norm_out[l, u, 1]))
            return gains + (w_gate[l, u].T, w_out[l, u].T)

        z_cur, ab_cols = [None] * CHUNKS, [None] * CHUNKS
        for p in range(CHUNKS):
            z_cur[p], ab = local_call(pair_rep, None, pair_mask, None, before(0), p, None, n_dev, width)
            ab_cols[p] = exchange(ab)
        out = None
        for s, (_, upd) in enumerate(steps):
            t_rows = []
            for q in range(CHUNKS):
                t_recv = exchange(tri_call(ab_cols, q, upd == 0))
                t_rows.append(t_recv.reshape(-1, *t_recv.shape[2:]))
            nxt = before(s + 1) if s + 1 < len(steps) else None
            new_ab = []
            for p in range(CHUNKS):
                res = local_call(z_cur[p], t_rows[p], pair_mask, after(s), nxt, p, out, n_dev, width)
                if nxt is None:
                    out = res
                else:
                    z_cur[p] = res[0]
                    new_ab.append(exchange(res[1]))
            ab_cols = new_ab
        return out

    return jax.shard_map(local_stack, mesh=mesh, in_specs=(row_spec, mask_spec, P(), P(), P(), P(), P()), out_specs=row_spec, check_vma=False)
```

```python
import functools

import jax
import jax.numpy as jnp
from jax import lax
from jax.experimental import pallas as pl
from jax.experimental.pallas import tpu as pltpu
from jax.sharding import PartitionSpec as P

LN_EPS = 1e-5
ROW_AXES = ("dap2", "dap")
ALL_ROWS = ("data", "dap2", "dap")
CHUNKS = 2
PIECES = 4
ROWS = 16
LANES = 128
F32, BF16 = jnp.float32, jnp.bfloat16


def channel_norm(values, gain, shift):
    mean_val = jnp.mean(values, axis=0, keepdims=True)
    centered = values - mean_val
    var_val = jnp.mean(centered * centered, axis=0, keepdims=True)
    return centered * lax.rsqrt(var_val + LN_EPS) * gain + shift


def sigmoid(values):
    return 1.0 / (1.0 + jnp.exp(-values))


def finish_and_project(refs, wts, scr, first, last):
    refs = list(refs)
    z_ref = refs.pop(0)
    t_ref = None if first else refs.pop(0)
    mask_ref = None if last else refs.pop(0)
    z_out = refs.pop(0)
    ab_out = None if last else refs.pop(0)
    if not first:
        gain_in, shift_in, gain_out, shift_out, wg_ref, wo_ref = wts[0]
    if not last:
        gain_nx, shift_nx, wab_ref = wts[1]
    t_scr, ab_scr = scr
    rows = z_ref.shape[0]
    cols = z_out.shape[1] if last else z_out.shape[2]
    blocks = cols // LANES
    hid = wab_ref.shape[0] // 4 if not last else wo_ref.shape[1]
    stride_t = t_scr.shape[1] // hid
    stride_ab = ab_scr.shape[1] // rows

    if not first:
        for blk in range(blocks):
            lanes = pl.ds(blk * LANES, LANES)

            def add_up(c, total):
                return total + t_ref[c, :, lanes].astype(F32)

            mean_val = lax.fori_loop(0, hid, add_up, jnp.zeros((rows, LANES), F32), unroll=8) * (1.0 / hid)

            def add_sq(c, total):
                centered = t_ref[c, :, lanes].astype(F32) - mean_val
                return total + centered * centered

            var_val = lax.fori_loop(0, hid, add_sq, jnp.zeros((rows, LANES), F32), unroll=8) * (1.0 / hid)
            scale = lax.rsqrt(var_val + LN_EPS)

            def put(c, carry):
                start = pl.multiple_of(c * stride_t, 8)
                t_scr[blk, pl.ds(start, rows), :] = (t_ref[c, :, lanes].astype(F32) - mean_val) * scale
                return carry

            lax.fori_loop(0, hid, put, 0, unroll=8)

    def one_row(r, carry):
        if first:
            z_val = z_ref[r].astype(F32).T.astype(BF16)
        else:
            z_val = z_ref[r]
        z_f = z_val.astype(F32)
        if not first:
            x_ln = channel_norm(z_f, gain_in[...], shift_in[...]).astype(BF16)
            t_n = [t_scr[blk, pl.ds(r, hid, stride=stride_t), :] for blk in range(blocks)]
            t_n = jnp.concatenate(t_n, axis=1) if blocks > 1 else t_n[0]
            y_ln = (t_n * gain_out[...] + shift_out[...]).astype(BF16)
            update_val = jnp.dot(wo_ref[...], y_ln, preferred_element_type=F32)
            gate_val = sigmoid(jnp.dot(wg_ref[...], x_ln, preferred_element_type=F32))
            z_f = z_f + gate_val * update_val
            if last:
                z_out[r] = z_f.T.astype(BF16)
                return carry
            z_val = z_f.astype(BF16)
            z_f = z_val.astype(F32)
        z_out[r] = z_val
        x_nx = channel_norm(z_f, gain_nx[...], shift_nx[...]).astype(BF16)
        m_row = mask_ref[pl.ds(r, 1), :].astype(F32)
        for half in range(2):
            proj = jnp.dot(wab_ref[pl.ds(half * 2 * hid, 2 * hid), :], x_nx, preferred_element_type=F32)
            val = m_row * sigmoid(proj[hid:]) * proj[:hid]
            start = pl.multiple_of(r * stride_ab + half * hid, 8)
            for blk in range(blocks):
                ab_scr[blk, pl.ds(start, hid), :] = val[:, blk * LANES : (blk + 1) * LANES]
        return carry

    lax.fori_loop(0, rows, one_row, 0)

    if not last:
        dests, per_dest = ab_out.shape[0], ab_out.shape[1] // 2

        def send_rows(d, carry):
            for half in range(2):
                for e in range(per_dest):
                    for blk in range(blocks):
                        val = ab_scr[blk, pl.ds(half * hid + d * per_dest + e, rows, stride=stride_ab), :]
                        ab_out[d, half * per_dest + e, :, pl.ds(blk * LANES, LANES)] = val.astype(BF16)
            return carry

        lax.fori_loop(0, dests, send_rows, 0)


def local_specs(chan, hid, n_dev, wb, nw, chunk, first, last):
    specs = [pl.BlockSpec((ROWS, wb, chan), lambda i, j: (i, chunk * nw + j, 0)) if first else pl.BlockSpec((ROWS, chan, wb), lambda i, j: (i, 0, j))]
    if not first:
        specs.append(pl.BlockSpec((hid, ROWS, wb), lambda i, j: (0, i, j)))
    if last:
        return specs, [pl.BlockSpec((ROWS, wb, chan), lambda i, j: (i, chunk * nw + j, 0))]
    specs.append(pl.BlockSpec((ROWS, wb), lambda i, j: (i, chunk * nw + j)))
    outs = [
        pl.BlockSpec((ROWS, chan, wb), lambda i, j: (i, 0, j)),
        pl.BlockSpec((n_dev, 2 * hid // n_dev, ROWS, wb), lambda i, j: (0, 0, i, j)),
    ]
    return specs, outs


def local_scratch(hid, wb):
    return [
        pltpu.VMEM((wb // LANES, hid * (ROWS + 8), LANES), F32),
        pltpu.VMEM((wb // LANES, ROWS * (2 * hid + 8), LANES), F32),
    ]


def local_call(z_in, t_in, mask_loc, prev, nxt, chunk, out_full, n_dev, width):
    first, last = prev is None, nxt is None
    rows_loc = mask_loc.shape[0]
    chan = z_in.shape[2] if first else z_in.shape[1]
    hid = chan if first else t_in.shape[0]
    wb = min(2 * LANES, width)
    nw = width // wb
    specs, out_specs = local_specs(chan, hid, n_dev, wb, nw, chunk, first, last)
    args = [z_in] + ([] if first else [t_in]) + ([] if last else [mask_loc])
    n_blocked = len(args)
    wts = list(prev or ()) + list(nxt or ())
    args += wts
    specs += [pl.BlockSpec(memory_space=pltpu.VMEM)] * len(wts)
    alias = {}
    if last:
        alias = {len(args): 0}
        args.append(out_full)
        specs.append(pl.BlockSpec(memory_space=pl.ANY))
        out_shape = [jax.ShapeDtypeStruct(out_full.shape, BF16)]
    else:
        out_shape = [
            jax.ShapeDtypeStruct((rows_loc, chan, width), BF16),
            jax.ShapeDtypeStruct((n_dev, 2 * hid // n_dev, rows_loc, width), BF16),
        ]

    def body(*refs):
        w_refs = refs[n_blocked : n_blocked + len(wts)]
        n_prev = len(prev or ())
        outs = refs[len(args) : len(args) + len(out_shape)]
        finish_and_project(refs[:n_blocked] + outs, (w_refs[:n_prev], w_refs[n_prev:]), refs[-2:], first, last)

    return pl.pallas_call(
        body,
        grid=(rows_loc // ROWS, nw),
        in_specs=specs,
        out_specs=out_specs,
        out_shape=out_shape,
        scratch_shapes=local_scratch(hid, wb),
        input_output_aliases=alias,
        compiler_params=pltpu.CompilerParams(vmem_limit_bytes=60 * 2**20),
        name=f"local_{chunk}",
    )(*args)


def out_kernel(*refs, chunks):
    t_ref = refs[-1]
    total = None
    for p in range(chunks):
        a_val = refs[p][...].reshape(-1, refs[p].shape[-1])
        b_val = refs[chunks + p][...].reshape(-1, refs[chunks + p].shape[-1])
        part = lax.dot_general(a_val, b_val, (((1,), (1,)), ((), ())), preferred_element_type=F32)
        total = part if total is None else total + part
    t_ref[...] = total.astype(BF16).reshape(t_ref.shape)


def in_kernel(*refs, chunks):
    b_ref, t_ref = refs[chunks], refs[-1]
    b_val = b_ref[...].reshape(-1, b_ref.shape[-1])
    n_dev, _, rows, _ = t_ref.shape
    share = n_dev // chunks
    for p in range(chunks):
        a_val = refs[p][...].reshape(-1, refs[p].shape[-1])
        part = lax.dot_general(a_val, b_val, (((0,), (0,)), ((), ())), preferred_element_type=F32)
        t_ref[p * share : (p + 1) * share] = part.astype(BF16).reshape(share, 1, rows, t_ref.shape[-1])


def offsets(nx, ny):
    signed = lambda n: [d if d <= n // 2 else d - n for d in range(n)]
    classes = {}
    for dx in signed(nx):
        for dy in signed(ny):
            if dx or dy:
                lo, hi = sorted((abs(dx), abs(dy)))
                classes.setdefault((lo != hi, lo, hi), []).append((dx, dy))
    return [sorted(classes[key], key=lambda o: (o[0] * o[1] < 0, o)) for key in sorted(classes)]


def start_exchange(src, dst, send_sem, recv_sem, self_sem, nx, ny, pieces):
    row, col = lax.axis_index("dap2"), lax.axis_index("dap")
    n_col = 2 * nx
    me = row * n_col + col
    chip, core = col // 2, lax.rem(col, 2)
    step = src.shape[1] // pieces

    def send(dx, dy, other, start, size):
        to_row = lax.rem(row + dy % ny, ny)
        to_col = lax.rem(chip + dx % nx, nx) * 2 + lax.rem(core + other, 2)
        pltpu.make_async_remote_copy(
            src_ref=src.at[to_row * n_col + to_col, pl.ds(start, size)],
            dst_ref=dst.at[me, pl.ds(start, size)],
            send_sem=send_sem,
            recv_sem=recv_sem,
            device_id={"dap2": to_row, "dap": to_col},
            device_id_type=pl.DeviceIdType.MESH,
        ).start()

    send(0, 0, 1, 0, src.shape[1])
    pltpu.make_async_copy(src.at[me], dst.at[me], self_sem).start()
    for group in offsets(nx, ny):

        def piece(h, carry):
            for other in range(2):
                for dx, dy in group:
                    send(dx, dy, other, h * step, step)
            return carry

        lax.fori_loop(0, pieces, piece, 0)


def wait_received(dst, recv_sem, self_sem):
    others = dst.at[pl.ds(0, dst.shape[0] - 1)]
    pltpu.make_async_copy(others, others, recv_sem).wait()
    pltpu.make_async_copy(dst.at[0], dst.at[0], self_sem).wait()


def wait_sent(src, send_sem):
    others = src.at[pl.ds(0, src.shape[0] - 1)]
    pltpu.make_async_copy(others, others, send_sem).wait()


def tri_specs(n_dev, per, rows, width, q, outgoing):
    a_spec = pl.BlockSpec((n_dev, 1, rows, width), lambda c: (0, c, 0, 0))
    if outgoing:
        b_specs = [pl.BlockSpec((n_dev // CHUNKS, 1, rows, width), lambda c: (q, per + c, 0, 0))] * CHUNKS
    else:
        b_specs = [pl.BlockSpec((n_dev, 1, rows, width), lambda c: (0, per + c, 0, 0))]
    return [a_spec] * CHUNKS + b_specs, [a_spec]


def update_call(ab0, z_cur, t_prev, mask_loc, prev, here, done, nxt, outgoing, first, last, mesh, cid):
    ny, nx = mesh.shape["dap2"], mesh.shape["dap"] // 2
    n_dev, per2, rows_loc, width = ab0.shape
    per = per2 // 2
    z0 = z_cur[0]
    chan, hid = z0.shape[1], per * n_dev
    wb = min(2 * LANES, width)
    nw = width // wb
    grid = (rows_loc // ROWS, nw)
    hbm = [ab0, z0, z_cur[1], mask_loc] + ([] if first else [t_prev])
    wts = list(prev or ()) + list(here) + list(done) + list(nxt or ())
    cuts = [len(prev or ()), len(here), len(done), len(nxt or ())]
    ab_type = jax.ShapeDtypeStruct(ab0.shape, BF16)
    t_type = jax.ShapeDtypeStruct((n_dev, per, rows_loc, width), BF16)
    z_type = jax.ShapeDtypeStruct((rows_loc, chan, width), BF16)
    out_type = jax.ShapeDtypeStruct((rows_loc, mask_loc.shape[1], chan), BF16)
    out_shape = [ab_type] * 3 + [t_type] * 4 + [z_type] + ([out_type] if last else [z_type, ab_type])

    def body(*refs):
        ins, w_refs = refs[: len(hbm)], refs[len(hbm) : len(hbm) + len(wts)]
        outs = refs[len(hbm) + len(wts) : len(hbm) + len(wts) + len(out_shape)]
        t_scr, ab_scr, send_sem, recv_sem, self_sem = refs[-5:]
        groups, at = [], 0
        for cut in cuts:
            groups.append(w_refs[at : at + cut])
            at += cut
        ab0_ref, z0_ref, z1_ref, mask_ref = ins[:4]
        ab1_ref, got0, got1, t0_ref, t1_ref, back0, back1, z1_out = outs[:8]
        scr = (t_scr, ab_scr)
        row, col = lax.axis_index("dap2"), lax.axis_index("dap")
        barrier = pltpu.get_barrier_semaphore()
        for k in range(1, n_dev):
            peer = {"dap2": lax.rem(row + k // (2 * nx), ny), "dap": lax.rem(col + k % (2 * nx), 2 * nx)}
            pl.semaphore_signal(barrier, inc=1, device_id=peer, device_id_type=pl.DeviceIdType.MESH)
        pl.semaphore_wait(barrier, n_dev - 1)

        def go(n, src, dst):
            start_exchange(src, dst, send_sem.at[n], recv_sem.at[n], self_sem.at[n], nx, ny, PIECES)

        def local(chunk, w_sets, fst, lst, *arrays):
            specs, out_specs = local_specs(chan, hid, n_dev, wb, nw, chunk, fst, lst)
            pltpu.emit_pipeline(
                lambda *blocks: finish_and_project(blocks, w_sets, scr, fst, lst),
                grid=grid,
                in_specs=specs,
                out_specs=out_specs,
            )(*arrays)

        def tri(q, t_ref):
            specs, out_specs = tri_specs(n_dev, per, rows_loc, width, q, outgoing)
            kernel = out_kernel if outgoing else in_kernel
            b_refs = [got0, got1] if outgoing else [(got0, got1)[q]]
            pltpu.emit_pipeline(
                lambda *blocks: kernel(*blocks, chunks=CHUNKS), grid=(per,), in_specs=specs, out_specs=out_specs
            )(got0, got1, *b_refs, t_ref)

        def rows_of(ref):
            return ref.reshape(hid, rows_loc, width)

        go(0, ab0_ref, got0)
        if first:
            local(1, (None, groups[1]), True, False, z1_ref, mask_ref, z1_out, ab1_ref)
        else:
            local(1, (groups[0], groups[1]), False, False, z1_ref, ins[4], mask_ref, z1_out, ab1_ref)
        go(1, ab1_ref, got1)
        wait_received(got0, recv_sem.at[0], self_sem.at[0])
        wait_received(got1, recv_sem.at[1], self_sem.at[1])
        tri(0, t0_ref)
        go(2, t0_ref, back0)
        tri(1, t1_ref)
        go(3, t1_ref, back1)
        wait_received(back0, recv_sem.at[2], self_sem.at[2])
        if last:
            local(0, (groups[2], None), False, True, z0_ref, rows_of(back0), outs[8])
        else:
            local(0, (groups[2], groups[3]), False, False, z0_ref, rows_of(back0), mask_ref, outs[8], outs[9])
        wait_received(back1, recv_sem.at[3], self_sem.at[3])
        for n, src in enumerate((ab0_ref, ab1_ref, t0_ref, t1_ref)):
            wait_sent(src, send_sem.at[n])

    res = pl.pallas_call(
        body,
        in_specs=[pl.BlockSpec(memory_space=pltpu.HBM)] * len(hbm) + [pl.BlockSpec(memory_space=pltpu.VMEM)] * len(wts),
        out_specs=[pl.BlockSpec(memory_space=pltpu.HBM)] * len(out_shape),
        out_shape=out_shape,
        scratch_shapes=local_scratch(hid, wb) + [pltpu.SemaphoreType.DMA((4,))] * 3,
        compiler_params=pltpu.CompilerParams(collective_id=cid, has_side_effects=True, vmem_limit_bytes=60 * 2**20),
        name=f"update_{cid}",
    )(*hbm, *wts)
    t1_rows = res[6].reshape(hid, rows_loc, width)
    if last:
        return res[8], res[7], t1_rows
    return res[9], [res[8], res[7]], t1_rows


def solution(mesh):
    n_dev = mesh.shape["dap2"] * mesh.shape["dap"]
    row_spec = P(ALL_ROWS, None, None)
    mask_spec = P(ALL_ROWS, None)

    def local_stack(pair_rep, pair_mask, norm_in, norm_out, w_ab, w_gate, w_out):
        width = pair_rep.shape[1] // CHUNKS
        wb = min(2 * LANES, width)

        def spread(vec):
            return jnp.broadcast_to(vec.astype(F32)[:, None], (vec.shape[0], wb))

        steps = [(layer, upd) for layer in range(w_ab.shape[0]) for upd in range(2)]

        def before(s):
            l, u = steps[s]
            return (spread(norm_in[l, u, 0]), spread(norm_in[l, u, 1]), w_ab[l, u].T)

        def after(s):
            l, u = steps[s]
            gains = tuple(spread(v) for v in (norm_in[l, u, 0], norm_in[l, u, 1], norm_out[l, u, 0], norm_out[l, u, 1]))
            return gains + (w_gate[l, u].T, w_out[l, u].T)

        z_first, ab0 = local_call(pair_rep, None, pair_mask, None, before(0), 0, None, n_dev, width)
        z_cur, t_prev = [z_first, pair_rep], None
        for s, (_, upd) in enumerate(steps):
            first, last = s == 0, s + 1 == len(steps)
            res = update_call(
                ab0, z_cur, t_prev, pair_mask, None if first else after(s - 1), before(s), after(s),
                None if last else before(s + 1), upd == 0, first, last, mesh, 1 + upd + (2 if last else 0) + (4 if first else 0),
            )
            if last:
                out, z_one, t_one = res
                return local_call(z_one, t_one, pair_mask, after(s), None, 1, out, n_dev, width)[0]
            ab0, z_cur, t_prev = res

    def mapped(*args):
        with jax.sharding.use_abstract_mesh(mesh.abstract_mesh):
            return jax.shard_map(local_stack, mesh=mesh, in_specs=(row_spec, mask_spec, P(), P(), P(), P(), P()), out_specs=row_spec, check_vma=False)(*args)

    return mapped
```

```python
import functools

import jax
import jax.numpy as jnp
from jax import lax
from jax.experimental import pallas as pl
from jax.experimental.pallas import tpu as pltpu
from jax.sharding import PartitionSpec as P

LN_EPS = 1e-5
ROW_AXES = ("dap2", "dap")
ALL_ROWS = ("data", "dap2", "dap")
CHUNKS = 2
PIECES = 4
ROWS = 16
LANES = 128
F32, BF16 = jnp.float32, jnp.bfloat16


def channel_norm(values, gain, shift):
    mean_val = jnp.mean(values, axis=0, keepdims=True)
    centered = values - mean_val
    var_val = jnp.mean(centered * centered, axis=0, keepdims=True)
    return centered * lax.rsqrt(var_val + LN_EPS) * gain + shift


def sigmoid(values):
    return 0.5 * jnp.tanh(0.5 * values) + 0.5


def finish_and_project(refs, wts, scr, first, last):
    refs = list(refs)
    z_ref = refs.pop(0)
    t_ref = None if first else refs.pop(0)
    mask_ref = None if last else refs.pop(0)
    z_out = refs.pop(0)
    ab_out = None if last else refs.pop(0)
    if not first:
        gain_in, shift_in, gain_out, shift_out, wg_ref, wo_ref = wts[0]
    if not last:
        gain_nx, shift_nx, wab_ref = wts[1]
    t_scr, ab_scr = scr
    rows = z_ref.shape[0]
    cols = z_out.shape[1] if last else z_out.shape[2]
    blocks = cols // LANES
    hid = wab_ref.shape[0] // 4 if not last else wo_ref.shape[1]
    stride_t = t_scr.shape[1] // hid
    stride_ab = ab_scr.shape[1] // rows

    if not first:
        for blk in range(blocks):
            lanes = pl.ds(blk * LANES, LANES)

            def add_up(c, total):
                return total + t_ref[c, :, lanes].astype(F32)

            mean_val = lax.fori_loop(0, hid, add_up, jnp.zeros((rows, LANES), F32), unroll=8) * (1.0 / hid)

            def add_sq(c, total):
                centered = t_ref[c, :, lanes].astype(F32) - mean_val
                return total + centered * centered

            var_val = lax.fori_loop(0, hid, add_sq, jnp.zeros((rows, LANES), F32), unroll=8) * (1.0 / hid)
            scale = lax.rsqrt(var_val + LN_EPS)

            def put(c, carry):
                start = pl.multiple_of(c * stride_t, 8)
                t_scr[blk, pl.ds(start, rows), :] = (t_ref[c, :, lanes].astype(F32) - mean_val) * scale
                return carry

            lax.fori_loop(0, hid, put, 0, unroll=8)

    def one_row(r, carry):
        if first:
            z_val = z_ref[r].astype(F32).T.astype(BF16)
        else:
            z_val = z_ref[r]
        z_f = z_val.astype(F32)
        if not first:
            x_ln = channel_norm(z_f, gain_in[...], shift_in[...]).astype(BF16)
            t_n = [t_scr[blk, pl.ds(r, hid, stride=stride_t), :] for blk in range(blocks)]
            t_n = jnp.concatenate(t_n, axis=1) if blocks > 1 else t_n[0]
            y_ln = (t_n * gain_out[...] + shift_out[...]).astype(BF16)
            update_val = jnp.dot(wo_ref[...], y_ln, preferred_element_type=F32)
            gate_val = sigmoid(jnp.dot(wg_ref[...], x_ln, preferred_element_type=F32))
            z_f = z_f + gate_val * update_val
            if last:
                z_out[r] = z_f.T.astype(BF16)
                return carry
            z_val = z_f.astype(BF16)
            z_f = z_val.astype(F32)
        z_out[r] = z_val
        x_nx = channel_norm(z_f, gain_nx[...], shift_nx[...]).astype(BF16)
        m_row = mask_ref[pl.ds(r, 1), :].astype(F32)
        for half in range(2):
            proj = jnp.dot(wab_ref[pl.ds(half * 2 * hid, 2 * hid), :], x_nx, preferred_element_type=F32)
            val = m_row * sigmoid(proj[hid:]) * proj[:hid]
            start = pl.multiple_of(r * stride_ab + half * hid, 8)
            for blk in range(blocks):
                ab_scr[blk, pl.ds(start, hid), :] = val[:, blk * LANES : (blk + 1) * LANES]
        return carry

    lax.fori_loop(0, rows, one_row, 0, unroll=4)

    if not last:
        dests, per_dest = ab_out.shape[0], ab_out.shape[1] // 2

        def send_rows(d, carry):
            for half in range(2):
                for e in range(per_dest):
                    for blk in range(blocks):
                        val = ab_scr[blk, pl.ds(half * hid + d * per_dest + e, rows, stride=stride_ab), :]
                        ab_out[d, half * per_dest + e, :, pl.ds(blk * LANES, LANES)] = val.astype(BF16)
            return carry

        lax.fori_loop(0, dests, send_rows, 0)


def local_specs(chan, hid, n_dev, wb, nw, chunk, first, last):
    specs = [pl.BlockSpec((ROWS, wb, chan), lambda i, j: (i, chunk * nw + j, 0)) if first else pl.BlockSpec((ROWS, chan, wb), lambda i, j: (i, 0, j))]
    if not first:
        specs.append(pl.BlockSpec((hid, ROWS, wb), lambda i, j: (0, i, j)))
    if last:
        return specs, [pl.BlockSpec((ROWS, wb, chan), lambda i, j: (i, chunk * nw + j, 0))]
    specs.append(pl.BlockSpec((ROWS, wb), lambda i, j: (i, chunk * nw + j)))
    outs = [
        pl.BlockSpec((ROWS, chan, wb), lambda i, j: (i, 0, j)),
        pl.BlockSpec((n_dev, 2 * hid // n_dev, ROWS, wb), lambda i, j: (0, 0, i, j)),
    ]
    return specs, outs


def local_scratch(hid, wb):
    return [
        pltpu.VMEM((wb // LANES, hid * (ROWS + 8), LANES), F32),
        pltpu.VMEM((wb // LANES, ROWS * (2 * hid + 8), LANES), F32),
    ]


def local_call(z_in, t_in, mask_loc, prev, nxt, chunk, out_full, n_dev, width):
    first, last = prev is None, nxt is None
    rows_loc = mask_loc.shape[0]
    chan = z_in.shape[2] if first else z_in.shape[1]
    hid = chan if first else t_in.shape[0]
    wb = min(2 * LANES, width)
    nw = width // wb
    specs, out_specs = local_specs(chan, hid, n_dev, wb, nw, chunk, first, last)
    args = [z_in] + ([] if first else [t_in]) + ([] if last else [mask_loc])
    n_blocked = len(args)
    wts = list(prev or ()) + list(nxt or ())
    args += wts
    specs += [pl.BlockSpec(memory_space=pltpu.VMEM)] * len(wts)
    alias = {}
    if last:
        alias = {len(args): 0}
        args.append(out_full)
        specs.append(pl.BlockSpec(memory_space=pl.ANY))
        out_shape = [jax.ShapeDtypeStruct(out_full.shape, BF16)]
    else:
        out_shape = [
            jax.ShapeDtypeStruct((rows_loc, chan, width), BF16),
            jax.ShapeDtypeStruct((n_dev, 2 * hid // n_dev, rows_loc, width), BF16),
        ]

    def body(*refs):
        w_refs = refs[n_blocked : n_blocked + len(wts)]
        n_prev = len(prev or ())
        outs = refs[len(args) : len(args) + len(out_shape)]
        finish_and_project(refs[:n_blocked] + outs, (w_refs[:n_prev], w_refs[n_prev:]), refs[-2:], first, last)

    return pl.pallas_call(
        body,
        grid=(rows_loc // ROWS, nw),
        in_specs=specs,
        out_specs=out_specs,
        out_shape=out_shape,
        scratch_shapes=local_scratch(hid, wb),
        input_output_aliases=alias,
        compiler_params=pltpu.CompilerParams(vmem_limit_bytes=60 * 2**20),
        name=f"local_{chunk}",
    )(*args)


def out_kernel(*refs, chunks):
    t_ref = refs[-1]
    total = None
    for p in range(chunks):
        a_val = refs[p][...].reshape(-1, refs[p].shape[-1])
        b_val = refs[chunks + p][...].reshape(-1, refs[chunks + p].shape[-1])
        part = lax.dot_general(a_val, b_val, (((1,), (1,)), ((), ())), preferred_element_type=F32)
        total = part if total is None else total + part
    t_ref[...] = total.astype(BF16).reshape(t_ref.shape)


def in_kernel(*refs, chunks):
    b_ref, t_ref = refs[chunks], refs[-1]
    b_val = b_ref[...].reshape(-1, b_ref.shape[-1])
    n_dev, _, rows, _ = t_ref.shape
    share = n_dev // chunks
    for p in range(chunks):
        a_val = refs[p][...].reshape(-1, refs[p].shape[-1])
        part = lax.dot_general(a_val, b_val, (((0,), (0,)), ((), ())), preferred_element_type=F32)
        t_ref[p * share : (p + 1) * share] = part.astype(BF16).reshape(share, 1, rows, t_ref.shape[-1])


def offsets(nx, ny):
    signed = lambda n: [d if d <= n // 2 else d - n for d in range(n)]
    classes = {}
    for dx in signed(nx):
        for dy in signed(ny):
            if dx or dy:
                lo, hi = sorted((abs(dx), abs(dy)))
                classes.setdefault((lo != hi, lo, hi), []).append((dx, dy))
    return [sorted(classes[key], key=lambda o: (o[0] * o[1] < 0, o)) for key in sorted(classes)]


def start_exchange(src, dst, send_sem, recv_sem, self_sem, nx, ny, pieces):
    row, col = lax.axis_index("dap2"), lax.axis_index("dap")
    n_col = 2 * nx
    me = row * n_col + col
    chip, core = col // 2, lax.rem(col, 2)
    step = src.shape[1] // pieces

    def send(dx, dy, other, start, size):
        to_row = lax.rem(row + dy % ny, ny)
        to_col = lax.rem(chip + dx % nx, nx) * 2 + lax.rem(core + other, 2)
        pltpu.make_async_remote_copy(
            src_ref=src.at[to_row * n_col + to_col, pl.ds(start, size)],
            dst_ref=dst.at[me, pl.ds(start, size)],
            send_sem=send_sem,
            recv_sem=recv_sem,
            device_id={"dap2": to_row, "dap": to_col},
            device_id_type=pl.DeviceIdType.MESH,
        ).start()

    send(0, 0, 1, 0, src.shape[1])
    pltpu.make_async_copy(src.at[me], dst.at[me], self_sem).start()
    for group in offsets(nx, ny):

        def piece(h, carry):
            for other in range(2):
                for dx, dy in group:
                    send(dx, dy, other, h * step, step)
            return carry

        lax.fori_loop(0, pieces, piece, 0)


def wait_received(dst, recv_sem, self_sem):
    others = dst.at[pl.ds(0, dst.shape[0] - 1)]
    pltpu.make_async_copy(others, others, recv_sem).wait()
    pltpu.make_async_copy(dst.at[0], dst.at[0], self_sem).wait()


def wait_sent(src, send_sem):
    others = src.at[pl.ds(0, src.shape[0] - 1)]
    pltpu.make_async_copy(others, others, send_sem).wait()


def tri_specs(n_dev, per, rows, width, q, outgoing):
    a_spec = pl.BlockSpec((n_dev, 1, rows, width), lambda c: (0, c, 0, 0))
    if outgoing:
        b_specs = [pl.BlockSpec((n_dev // CHUNKS, 1, rows, width), lambda c: (q, per + c, 0, 0))] * CHUNKS
    else:
        b_specs = [pl.BlockSpec((n_dev, 1, rows, width), lambda c: (0, per + c, 0, 0))]
    return [a_spec] * CHUNKS + b_specs, [a_spec]


def update_call(ab0, z_cur, t_prev, mask_loc, prev, here, done, nxt, outgoing, first, last, mesh, cid):
    ny, nx = mesh.shape["dap2"], mesh.shape["dap"] // 2
    n_dev, per2, rows_loc, width = ab0.shape
    per = per2 // 2
    z0 = z_cur[0]
    chan, hid = z0.shape[1], per * n_dev
    wb = min(2 * LANES, width)
    nw = width // wb
    grid = (rows_loc // ROWS, nw)
    hbm = [ab0, z0, z_cur[1], mask_loc] + ([] if first else [t_prev])
    wts = list(prev or ()) + list(here) + list(done) + list(nxt or ())
    cuts = [len(prev or ()), len(here), len(done), len(nxt or ())]
    ab_type = jax.ShapeDtypeStruct(ab0.shape, BF16)
    t_type = jax.ShapeDtypeStruct((n_dev, per, rows_loc, width), BF16)
    z_type = jax.ShapeDtypeStruct((rows_loc, chan, width), BF16)
    out_type = jax.ShapeDtypeStruct((rows_loc, mask_loc.shape[1], chan), BF16)
    out_shape = [ab_type] * 3 + [t_type] * 4 + [z_type] + ([out_type] if last else [z_type, ab_type])

    def body(*refs):
        ins, w_refs = refs[: len(hbm)], refs[len(hbm) : len(hbm) + len(wts)]
        outs = refs[len(hbm) + len(wts) : len(hbm) + len(wts) + len(out_shape)]
        t_scr, ab_scr, send_sem, recv_sem, self_sem = refs[-5:]
        groups, at = [], 0
        for cut in cuts:
            groups.append(w_refs[at : at + cut])
            at += cut
        ab0_ref, z0_ref, z1_ref, mask_ref = ins[:4]
        ab1_ref, got0, got1, t0_ref, t1_ref, back0, back1, z1_out = outs[:8]
        scr = (t_scr, ab_scr)
        row, col = lax.axis_index("dap2"), lax.axis_index("dap")
        barrier = pltpu.get_barrier_semaphore()
        for k in range(1, n_dev):
            peer = {"dap2": lax.rem(row + k // (2 * nx), ny), "dap": lax.rem(col + k % (2 * nx), 2 * nx)}
            pl.semaphore_signal(barrier, inc=1, device_id=peer, device_id_type=pl.DeviceIdType.MESH)
        pl.semaphore_wait(barrier, n_dev - 1)

        def go(n, src, dst):
            start_exchange(src, dst, send_sem.at[n], recv_sem.at[n], self_sem.at[n], nx, ny, PIECES)

        def local(chunk, w_sets, fst, lst, *arrays):
            specs, out_specs = local_specs(chan, hid, n_dev, wb, nw, chunk, fst, lst)
            pltpu.emit_pipeline(
                lambda *blocks: finish_and_project(blocks, w_sets, scr, fst, lst),
                grid=grid,
                in_specs=specs,
                out_specs=out_specs,
            )(*arrays)

        def tri(q, t_ref):
            specs, out_specs = tri_specs(n_dev, per, rows_loc, width, q, outgoing)
            kernel = out_kernel if outgoing else in_kernel
            b_refs = [got0, got1] if outgoing else [(got0, got1)[q]]
            pltpu.emit_pipeline(
                lambda *blocks: kernel(*blocks, chunks=CHUNKS), grid=(per,), in_specs=specs, out_specs=out_specs
            )(got0, got1, *b_refs, t_ref)

        def rows_of(ref):
            return ref.reshape(hid, rows_loc, width)

        go(0, ab0_ref, got0)
        if first:
            local(1, (None, groups[1]), True, False, z1_ref, mask_ref, z1_out, ab1_ref)
        else:
            local(1, (groups[0], groups[1]), False, False, z1_ref, ins[4], mask_ref, z1_out, ab1_ref)
        go(1, ab1_ref, got1)
        wait_received(got0, recv_sem.at[0], self_sem.at[0])
        wait_received(got1, recv_sem.at[1], self_sem.at[1])
        tri(0, t0_ref)
        go(2, t0_ref, back0)
        tri(1, t1_ref)
        go(3, t1_ref, back1)
        wait_received(back0, recv_sem.at[2], self_sem.at[2])
        if last:
            local(0, (groups[2], None), False, True, z0_ref, rows_of(back0), outs[8])
        else:
            local(0, (groups[2], groups[3]), False, False, z0_ref, rows_of(back0), mask_ref, outs[8], outs[9])
        wait_received(back1, recv_sem.at[3], self_sem.at[3])
        for n, src in enumerate((ab0_ref, ab1_ref, t0_ref, t1_ref)):
            wait_sent(src, send_sem.at[n])

    res = pl.pallas_call(
        body,
        in_specs=[pl.BlockSpec(memory_space=pltpu.HBM)] * len(hbm) + [pl.BlockSpec(memory_space=pltpu.VMEM)] * len(wts),
        out_specs=[pl.BlockSpec(memory_space=pltpu.HBM)] * len(out_shape),
        out_shape=out_shape,
        scratch_shapes=local_scratch(hid, wb) + [pltpu.SemaphoreType.DMA((4,))] * 3,
        compiler_params=pltpu.CompilerParams(collective_id=cid, has_side_effects=True, vmem_limit_bytes=60 * 2**20),
        name=f"update_{cid}",
    )(*hbm, *wts)
    t1_rows = res[6].reshape(hid, rows_loc, width)
    if last:
        return res[8], res[7], t1_rows
    return res[9], [res[8], res[7]], t1_rows


def solution(mesh):
    n_dev = mesh.shape["dap2"] * mesh.shape["dap"]
    row_spec = P(ALL_ROWS, None, None)
    mask_spec = P(ALL_ROWS, None)

    def local_stack(pair_rep, pair_mask, norm_in, norm_out, w_ab, w_gate, w_out):
        width = pair_rep.shape[1] // CHUNKS
        wb = min(2 * LANES, width)

        def spread(vec):
            return jnp.broadcast_to(vec.astype(F32)[:, None], (vec.shape[0], wb))

        steps = [(layer, upd) for layer in range(w_ab.shape[0]) for upd in range(2)]

        def before(s):
            l, u = steps[s]
            return (spread(norm_in[l, u, 0]), spread(norm_in[l, u, 1]), w_ab[l, u].T)

        def after(s):
            l, u = steps[s]
            gains = tuple(spread(v) for v in (norm_in[l, u, 0], norm_in[l, u, 1], norm_out[l, u, 0], norm_out[l, u, 1]))
            return gains + (w_gate[l, u].T, w_out[l, u].T)

        z_first, ab0 = local_call(pair_rep, None, pair_mask, None, before(0), 0, None, n_dev, width)
        z_cur, t_prev = [z_first, pair_rep], None
        for s, (_, upd) in enumerate(steps):
            first, last = s == 0, s + 1 == len(steps)
            res = update_call(
                ab0, z_cur, t_prev, pair_mask, None if first else after(s - 1), before(s), after(s),
                None if last else before(s + 1), upd == 0, first, last, mesh, 1 + upd + (2 if last else 0) + (4 if first else 0),
            )
            if last:
                out, z_one, t_one = res
                return local_call(z_one, t_one, pair_mask, after(s), None, 1, out, n_dev, width)[0]
            ab0, z_cur, t_prev = res

    def mapped(*args):
        with jax.sharding.use_abstract_mesh(mesh.abstract_mesh):
            return jax.shard_map(local_stack, mesh=mesh, in_specs=(row_spec, mask_spec, P(), P(), P(), P(), P()), out_specs=row_spec, check_vma=False)(*args)

    return mapped
```
